32 devices in a mesh: owner: 4 (over x, core), rows: 8 (over z, y).
Axes of the slice: x: 2, y: 2, z: 4, core: 2. Of those that a mesh axis runs over, the one named last changes fastest.
Arguments:
- master_gate: float32 [64, 2048, 1408], P('owner', 'rows'), may hold values from -0.1875 to 0.1875
- master_up: float32 [64, 2048, 1408], P('owner', 'rows'), may hold values from -0.1875 to 0.1875
- router_weight: float32 [2048, 64], P('rows', 'owner'), may hold values from -0.125 to 0.125
- router_gain: float32 [2048], P('rows'), may hold values from 0.25 to 1.75
Outputs:
- final_gate: bfloat16 [64, 2048, 1408], P('owner', None, 'rows')
- final_up: bfloat16 [64, 2048, 1408], P('owner', None, 'rows')
- scale_gate: float32 [64, 1408], P('owner', 'rows')
- scale_up: float32 [64, 1408], P('owner', 'rows')
- serve_router: bfloat16 [2048, 64], replicated
The draws below stay inside these ranges and needn't reach their ends.
All inputs are finite; a program needn't handle non-finite values. Where the reference program divides by a largest or mean magnitude, that divisor is 1e-20 or more.
Results may differ from the reference program's by a relative error of at most 0.001.
Values may be sent and summed in bfloat16 or wider, within the bound.
A program may use at most 192 MiB of HBM per device.

```python
import jax
import jax.numpy as jnp

EXPERTS = 64
D_MODEL = 2048
D_EXPERT = 1408


def strengthened(entries, key, source, target, blocks, factor):
    owner, partner = [(jnp.arange(entries.shape[dim]) // (entries.shape[dim] // blocks)).reshape([-1 if axis == dim else 1 for axis in range(entries.ndim)]) for dim in (source, target)]
    chosen = jax.random.permutation(key, blocks)[partner]
    strong = (owner == chosen) | (owner == (partner + blocks // 2) % blocks)
    return jnp.where(strong, factor * entries, entries)


def levels(stream_key, dims, pieces, low, largest):
    level = 1.0
    for position, shards_of in pieces:
        steps = jax.random.uniform(jax.random.fold_in(jax.random.fold_in(stream_key, 6), position), (shards_of,), jnp.float32, low / len(pieces), largest / len(pieces))
        level = level * jnp.repeat(jnp.exp(steps), dims[position] // shards_of).reshape((-1,) + (1,) * (len(dims) - 1 - position))
    return level


def centred(rng, extent, spread, limit, shards=(), dtype=jnp.bfloat16):
    result = spread * jax.random.normal(rng, extent, jnp.float32)
    if shards:
        result = result * levels(rng, extent, shards, -0.22, 0.18)
    return jnp.clip(result, -limit, limit).astype(dtype)


def gaussian_with(own_key, shape, scale, bound, cuts, heavy, dtype=jnp.bfloat16):
    drawn = scale * jax.random.normal(own_key, shape, jnp.float32)
    if cuts:
        drawn = drawn * levels(own_key, shape, cuts, -0.22, 0.18)
    return jnp.clip(strengthened(drawn, jax.random.fold_in(own_key, 3), *heavy), -bound, bound).astype(dtype)


def setup_inputs(seed: int = 0) -> dict:
    streams_of = jax.random.split(jax.random.key(seed), 5)
    return {
        "master_gate": gaussian_with(streams_of[0], (EXPERTS, D_MODEL, D_EXPERT), D_MODEL ** -0.5, 0.1875, ((0, 4), (1, 8)), (1, 2, 8, 2.0), jnp.float32),
        "master_up": gaussian_with(streams_of[1], (EXPERTS, D_MODEL, D_EXPERT), D_MODEL ** -0.5, 0.1875, ((0, 4), (1, 8)), (1, 2, 8, 2.0), jnp.float32),
        "router_weight": centred(streams_of[2], (D_MODEL, EXPERTS), D_MODEL ** -0.5, 0.125, ((0, 8), (1, 4)), jnp.float32),
        "router_gain": jnp.clip(1.0 + 0.15 * jax.random.normal(streams_of[3], (D_MODEL,), jnp.float32), 0.25, 1.75),
    }


def reference(master_gate, master_up, router_weight, router_gain):
    scale_gate = jnp.max(jnp.abs(master_gate), axis=1)
    final_gate = (master_gate / jnp.expand_dims(scale_gate, 1)).astype(jnp.bfloat16)
    scale_up = jnp.max(jnp.abs(master_up), axis=1)
    final_up = (master_up / jnp.expand_dims(scale_up, 1)).astype(jnp.bfloat16)
    serve_router = (router_weight * router_gain[:, None]).astype(jnp.bfloat16)
    return final_gate, final_up, scale_gate, scale_up, serve_router
```

```python
import functools

import jax
import jax.numpy as jnp
from jax import lax
from jax.experimental import pallas as pl
from jax.experimental.pallas import tpu as pltpu
from jax.sharding import PartitionSpec as P

MESH = pl.DeviceIdType.MESH
LANES = 128
SUBLANES = 8
PACKED = 16
SLOTS = 4
PER_SEND = 2
VMEM_FOR_BLOCKS = 48 * 1024 * 1024


def kernel(
    owners,
    peers,
    gate,
    up,
    router,
    gain,
    out_gate,
    out_up,
    out_router,
    scales,
    slots,
    largest,
    parts,
    send,
    row,
    slot_sem,
    send_sem,
    recv_sem,
    part_send,
    part_recv,
    whole_send,
    whole_recv,
    router_send,
    router_recv,
):
    owner, me = lax.axis_index("owner"), lax.axis_index("rows")
    experts, rows, width = gate.shape
    tiles = width // LANES
    cut = width // peers
    per = parts.shape[1]
    masters, outs = (gate, up), (out_gate, out_up)

    def fetch(m, e):
        s = lax.rem(e, SLOTS)
        return pltpu.make_async_copy(masters[m].at[e], slots.at[m, s], slot_sem.at[m, s])

    for m in range(2):
        for e in range(SLOTS):
            fetch(m, e).start()

    lanes = pl.ds(pl.multiple_of(me * rows, LANES), rows)
    depth = router.shape[0]
    block = out_router.at[pl.ds(pl.multiple_of(owner * depth, PACKED), depth), lanes]
    row[...] = (router[...] * gain[...]).astype(row.dtype)
    flat = owner * peers + me
    count = owners * peers

    def router_copy(k):
        to = lax.rem(flat + k, count)
        return pltpu.make_async_remote_copy(
            src_ref=row,
            dst_ref=block,
            send_sem=router_send.at[k],
            recv_sem=router_recv.at[k],
            device_id={"owner": to // peers, "rows": lax.rem(to, peers)},
            device_id_type=MESH,
        )

    largest[...] = jnp.zeros_like(largest)
    for m in range(2):

        def maxima(e, _, m=m):
            fetch(m, e).wait()
            k = m * experts + e
            for c in range(tiles):
                x = slots[m, lax.rem(e, SLOTS), :, c * LANES : (c + 1) * LANES]
                largest[(k // SUBLANES) * tiles + c, pl.ds(lax.rem(k, SUBLANES), 1), :] = jnp.max(
                    jnp.abs(x), axis=0, keepdims=True
                )
            fetch(m, lax.rem(e + SLOTS, experts)).start()
            return 0

        lax.fori_loop(0, experts, maxima, 0)

    def part_copy(k):
        to = lax.rem(me + k, peers)
        return pltpu.make_async_remote_copy(
            src_ref=largest.at[pl.ds(to * per, per)],
            dst_ref=parts.at[k],
            send_sem=part_send.at[k],
            recv_sem=part_recv.at[k],
            device_id={"rows": to},
            device_id_type=MESH,
        )

    mine = scales.at[pl.ds(me * per, per)]

    def whole_copy(k):
        return pltpu.make_async_remote_copy(
            src_ref=mine,
            dst_ref=mine,
            send_sem=whole_send.at[k],
            recv_sem=whole_recv.at[k],
            device_id={"rows": lax.rem(me + k, peers)},
            device_id_type=MESH,
        )

    for k in range(1, peers):
        part_copy(k).start()
    total = largest[pl.ds(me * per, per)]
    for k in range(1, peers):
        part_copy(k).wait_recv()
        total = jnp.maximum(total, parts[k])
    mine[...] = total
    for k in range(1, peers):
        whole_copy(k).start()
    for k in range(1, peers):
        part_copy(k).wait_send()
    for k in range(1, peers):
        there = scales.at[pl.ds(lax.rem(me + peers - k, peers) * per, per)]
        pltpu.make_async_copy(there, there, whole_recv.at[k]).wait()
    for k in range(1, peers):
        whole_copy(k).wait_send()

    def send_copy(m, k, e, length):
        to = lax.rem(me + k, peers)
        return pltpu.make_async_remote_copy(
            src_ref=send.at[m, pl.ds(e, length), pl.ds(pl.multiple_of(to * cut, PACKED), cut), :],
            dst_ref=outs[m].at[pl.ds(e, length), :, lanes],
            send_sem=send_sem.at[m, k],
            recv_sem=recv_sem.at[m, k],
            device_id={"rows": to},
            device_id_type=MESH,
        )

    def keep_copy(m, e, length):
        return pltpu.make_async_copy(
            send.at[m, pl.ds(e, length), pl.ds(pl.multiple_of(me * cut, PACKED), cut), :],
            outs[m].at[pl.ds(e, length), :, lanes],
            send_sem.at[m, 0],
        )

    order = sorted(range(1, peers), key=lambda k: abs(2 * k - peers))
    for m in range(2):

        def bulk(step, _, m=m):
            for i in range(PER_SEND):
                e = step * PER_SEND + i
                fetch(m, e).wait()
                k = m * experts + e
                for c in range(tiles):
                    x = slots[m, lax.rem(e, SLOTS), :, c * LANES : (c + 1) * LANES]
                    s = scales[(k // SUBLANES) * tiles + c, pl.ds(lax.rem(k, SUBLANES), 1), :]
                    send[m, e, c * LANES : (c + 1) * LANES, :] = (x / s).T.astype(send.dtype)

                @pl.when(e + SLOTS < experts)
                def _(e=e):
                    fetch(m, e + SLOTS).start()

            for k in order:
                send_copy(m, k, step * PER_SEND, PER_SEND).start()
            keep_copy(m, step * PER_SEND, PER_SEND).start()
            return 0

        lax.fori_loop(0, experts // PER_SEND, bulk, 0)
        if m == 0:

            def router_start(k, _):
                router_copy(k).start()
                return 0

            lax.fori_loop(1, count, router_start, 0)
            pltpu.make_async_copy(row, block, router_send.at[0]).start()

    pltpu.make_async_copy(row, block, router_send.at[0]).wait()

    def router_wait(k, _):
        router_copy(k).wait()
        return 0

    lax.fori_loop(1, count, router_wait, 0)
    for m in range(2):
        keep_copy(m, 0, experts).wait()
        for k in range(1, peers):
            send_copy(m, k, 0, experts).wait()


def fused(owners, peers, master_gate, master_up, router_weight, router_gain):
    experts, rows, width = master_gate.shape
    cut = width // peers
    tiles = width // LANES
    groups = 2 * experts // SUBLANES
    per = -(-groups * tiles // peers)
    depth = router_weight.shape[1]
    anywhere = pl.BlockSpec(memory_space=pl.ANY)
    vmem = pl.BlockSpec(memory_space=pltpu.VMEM)
    dma = pltpu.SemaphoreType.DMA
    turned = jax.ShapeDtypeStruct((experts, cut, rows * peers), jnp.bfloat16)
    gate, up, router, scales = pl.pallas_call(
        functools.partial(kernel, owners, peers),
        out_shape=(
            turned,
            turned,
            jax.ShapeDtypeStruct((depth * owners, rows * peers), jnp.bfloat16),
            jax.ShapeDtypeStruct((per * peers, SUBLANES, LANES), jnp.float32),
        ),
        in_specs=[anywhere, anywhere, vmem, vmem],
        out_specs=(anywhere, anywhere, anywhere, vmem),
        scratch_shapes=[
            pltpu.VMEM((2, SLOTS, rows, width), jnp.float32),
            pltpu.VMEM((per * peers, SUBLANES, LANES), jnp.float32),
            pltpu.VMEM((peers, per, SUBLANES, LANES), jnp.float32),
            pltpu.VMEM((2, experts, width, rows), jnp.bfloat16),
            pltpu.VMEM((depth, rows), jnp.bfloat16),
            dma((2, SLOTS)),
            dma((2, peers)),
            dma((2, peers)),
            dma((peers,)),
            dma((peers,)),
            dma((peers,)),
            dma((peers,)),
            dma((owners * peers,)),
            dma((owners * peers,)),
        ],
        compiler_params=pltpu.CompilerParams(
            has_side_effects=True, vmem_limit_bytes=60 * 1024 * 1024
        ),
    )(master_gate, master_up, router_weight.T, router_gain[None, :])
    scales = scales[: groups * tiles].reshape(2, experts // SUBLANES, tiles, SUBLANES, LANES)
    scales = scales.transpose(0, 1, 3, 2, 4).reshape(2, experts, width)
    scales = lax.dynamic_slice_in_dim(scales, lax.axis_index("rows") * cut, cut, axis=2)
    return (
        gate.transpose(0, 2, 1),
        up.transpose(0, 2, 1),
        scales[0],
        scales[1],
        router.T,
    )


def plain(master_gate, master_up, router_weight, router_gain):
    scale_gate, scale_up = lax.pmax(
        (jnp.max(jnp.abs(master_gate), axis=1), jnp.max(jnp.abs(master_up), axis=1)), "rows"
    )
    narrow_gate, narrow_up = (
        (master_gate / jnp.expand_dims(scale_gate, 1)).astype(jnp.bfloat16),
        (master_up / jnp.expand_dims(scale_up, 1)).astype(jnp.bfloat16),
    )
    final_gate, final_up = (
        lax.all_to_all(narrow_gate, "rows", split_axis=2, concat_axis=1, tiled=True),
        lax.all_to_all(narrow_up, "rows", split_axis=2, concat_axis=1, tiled=True),
    )
    scale_gate = lax.dynamic_slice_in_dim(
        scale_gate, lax.axis_index("rows") * final_gate.shape[2], final_gate.shape[2], axis=1
    )
    scale_up = lax.dynamic_slice_in_dim(
        scale_up, lax.axis_index("rows") * final_up.shape[2], final_up.shape[2], axis=1
    )
    part_router = (router_weight * router_gain[:, None]).astype(jnp.bfloat16)
    row_router = lax.all_gather(part_router, "rows", axis=0, tiled=True)
    serve_router = lax.all_gather(row_router, "owner", axis=1, tiled=True)
    return (final_gate, final_up, scale_gate, scale_up, serve_router)


def solution(mesh):
    owners, peers = mesh.shape["owner"], mesh.shape["rows"]

    def shards(master_gate, master_up, router_weight, router_gain):
        experts, rows, width = master_gate.shape
        whole_tiles = (
            rows % LANES == 0
            and width % LANES == 0
            and width % (peers * PACKED) == 0
            and experts % SUBLANES == 0
            and experts % SLOTS == 0
            and experts % PER_SEND == 0
            and router_weight.shape[1] % PACKED == 0
            and (4 * experts + 8 * SLOTS) * rows * width <= VMEM_FOR_BLOCKS
        )
        run = functools.partial(fused, owners, peers) if whole_tiles else plain
        return run(master_gate, master_up, router_weight, router_gain)

    return jax.shard_map(
        shards,
        mesh=mesh,
        in_specs=(
            P("owner", "rows", None),
            P("owner", "rows", None),
            P("rows", "owner"),
            P("rows"),
        ),
        out_specs=(
            P("owner", None, "rows"),
            P("owner", None, "rows"),
            P("owner", "rows"),
            P("owner", "rows"),
            P(),
        ),
        check_vma=False,
    )
```

```python
import functools

import jax
import jax.numpy as jnp
from jax import lax
from jax.experimental import pallas as pl
from jax.experimental.pallas import tpu as pltpu
from jax.sharding import PartitionSpec as P

MESH = pl.DeviceIdType.MESH
LANES = 128
SUBLANES = 8
PACKED = 16
SLOTS = 4
PER_SEND = 2
VMEM_FOR_BLOCKS = 48 * 1024 * 1024
VMEM_FOR_REST = 2 * 1024 * 1024


def kernel(
    owners,
    peers,
    gate,
    up,
    router,
    gain,
    out_gate,
    out_up,
    out_router,
    scales_first,
    scales_rest,
    slots,
    largest_first,
    largest_rest,
    parts_first,
    parts_rest,
    send,
    row,
    slot_sem,
    send_sem,
    recv_sem,
    part_send,
    part_recv,
    whole_send,
    whole_recv,
    router_send,
    router_recv,
):
    owner, me = lax.axis_index("owner"), lax.axis_index("rows")
    experts, rows, width = gate.shape
    tiles = width // LANES
    cut = width // peers
    masters, outs = (gate, up), (out_gate, out_up)
    largest, parts = (largest_first, largest_rest), (parts_first, parts_rest)
    scales = (scales_first, scales_rest)
    lanes = pl.ds(pl.multiple_of(me * rows, LANES), rows)

    def fetch(m, first, i):
        s = lax.rem(i, SLOTS)
        return pltpu.make_async_copy(masters[m].at[first + i], slots.at[s], slot_sem.at[s])

    def begin(m, first, length):
        for i in range(min(SLOTS, length)):
            fetch(m, first, i).start()

    def advance(m, first, length, i):
        if length > SLOTS:

            @pl.when(i + SLOTS < length)
            def _():
                fetch(m, first, i + SLOTS).start()

    def place(m, e, c, first):
        k = m * experts + e - (0 if first else SUBLANES)
        return (k // SUBLANES) * tiles + c, pl.ds(lax.rem(k, SUBLANES), 1)

    def maxima(m, first, length):
        stage = 0 if m == 0 and first < SUBLANES else 1

        def body(i, _):
            fetch(m, first, i).wait()
            for c in range(tiles):
                x = slots[lax.rem(i, SLOTS), :, c * LANES : (c + 1) * LANES]
                tile, sub = place(m, first + i, c, stage == 0)
                largest[stage][tile, sub, :] = jnp.max(jnp.abs(x), axis=0, keepdims=True)
            advance(m, first, length, i)
            return 0

        lax.fori_loop(0, length, body, 0)

    def part_copy(stage, k):
        per = parts[stage].shape[1]
        to = lax.rem(me + k, peers)
        return pltpu.make_async_remote_copy(
            src_ref=largest[stage].at[pl.ds(to * per, per)],
            dst_ref=parts[stage].at[k],
            send_sem=part_send.at[stage, k],
            recv_sem=part_recv.at[stage, k],
            device_id={"rows": to},
            device_id_type=MESH,
        )

    def share(stage, of):
        per = parts[stage].shape[1]
        return scales[stage].at[pl.ds(of * per, per)]

    def whole_copy(stage, k):
        return pltpu.make_async_remote_copy(
            src_ref=share(stage, me),
            dst_ref=share(stage, me),
            send_sem=whole_send.at[stage, k],
            recv_sem=whole_recv.at[stage, k],
            device_id={"rows": lax.rem(me + k, peers)},
            device_id_type=MESH,
        )

    order = sorted(range(1, peers), key=lambda k: abs(2 * k - peers))

    def scatter(stage):
        for k in order:
            part_copy(stage, k).start()

    def reduce(stage):
        per = parts[stage].shape[1]
        total = largest[stage][pl.ds(me * per, per)]
        for k in order:
            part_copy(stage, k).wait_recv()
            total = jnp.maximum(total, parts[stage][k])
        share(stage, me)[...] = total
        for k in order:
            whole_copy(stage, k).start()

    def gathered(stage):
        for k in order:
            part_copy(stage, k).wait_send()
            there = share(stage, lax.rem(me + peers - k, peers))
            pltpu.make_async_copy(there, there, whole_recv.at[stage, k]).wait()
            whole_copy(stage, k).wait_send()

    def send_copy(m, k, e, length):
        to = lax.rem(me + k, peers)
        return pltpu.make_async_remote_copy(
            src_ref=send.at[m, pl.ds(e, length), pl.ds(pl.multiple_of(to * cut, PACKED), cut), :],
            dst_ref=outs[m].at[pl.ds(e, length), :, lanes],
            send_sem=send_sem.at[m, k],
            recv_sem=recv_sem.at[m, k],
            device_id={"rows": to},
            device_id_type=MESH,
        )

    def keep_copy(m, e, length):
        return pltpu.make_async_copy(
            send.at[m, pl.ds(e, length), pl.ds(pl.multiple_of(me * cut, PACKED), cut), :],
            outs[m].at[pl.ds(e, length), :, lanes],
            send_sem.at[m, 0],
        )

    def bulk(m, first, length, batch):
        stage = 0 if m == 0 and first < SUBLANES else 1

        def body(step, _):
            for j in range(batch):
                i = step * batch + j
                fetch(m, first, i).wait()
                for c in range(tiles):
                    x = slots[lax.rem(i, SLOTS), :, c * LANES : (c + 1) * LANES]
                    tile, sub = place(m, first + i, c, stage == 0)
                    s = scales[stage][tile, sub, :]
                    send[m, first + i, c * LANES : (c + 1) * LANES, :] = (x / s).T.astype(send.dtype)
                advance(m, first, length, i)
            for k in order:
                send_copy(m, k, first + step * batch, batch).start()
            keep_copy(m, first + step * batch, batch).start()
            return 0

        lax.fori_loop(0, length // batch, body, 0)

    depth = router.shape[0]
    block = out_router.at[pl.ds(pl.multiple_of(owner * depth, PACKED), depth), lanes]
    flat = owner * peers + me
    count = owners * peers

    def router_copy(k):
        to = lax.rem(flat + k, count)
        return pltpu.make_async_remote_copy(
            src_ref=row,
            dst_ref=block,
            send_sem=router_send.at[k],
            recv_sem=router_recv.at[k],
            device_id={"owner": to // peers, "rows": lax.rem(to, peers)},
            device_id_type=MESH,
        )

    def router_start(k, _):
        router_copy(k).start()
        return 0

    def router_wait(k, _):
        router_copy(k).wait()
        return 0

    begin(0, 0, SUBLANES)
    largest_first[...] = jnp.zeros_like(largest_first)
    largest_rest[...] = jnp.zeros_like(largest_rest)
    row[...] = (router[...] * gain[...]).astype(row.dtype)
    maxima(0, 0, SUBLANES)
    scatter(0)
    begin(0, 0, 2)
    reduce(0)
    gathered(0)
    bulk(0, 0, 2, 1)
    if experts > SUBLANES:
        begin(0, SUBLANES, experts - SUBLANES)
        maxima(0, SUBLANES, experts - SUBLANES)
    begin(1, 0, experts)
    maxima(1, 0, experts)
    scatter(1)
    begin(0, 2, 2)
    bulk(0, 2, 2, 2)
    begin(0, 4, SUBLANES - 4)
    reduce(1)
    bulk(0, 4, SUBLANES - 4, PER_SEND)
    if experts > SUBLANES:
        begin(0, SUBLANES, experts - SUBLANES)
    gathered(1)
    if experts > SUBLANES:
        bulk(0, SUBLANES, experts - SUBLANES, PER_SEND)
    begin(1, 0, experts)
    lax.fori_loop(1, count, router_start, 0)
    keep_router = pltpu.make_async_copy(row, block, router_send.at[0])
    keep_router.start()
    bulk(1, 0, experts, PER_SEND)

    keep_router.wait()
    lax.fori_loop(1, count, router_wait, 0)
    for m in range(2):
        keep_copy(m, 0, experts).wait()
        for k in range(1, peers):
            send_copy(m, k, 0, experts).wait()


def land(*refs):
    arrays = len(refs) // 2
    ins, outs, sem = refs[:arrays], refs[arrays:-1], refs[-1]
    copies = [pltpu.make_async_copy(a, b, sem.at[i]) for i, (a, b) in enumerate(zip(ins, outs))]
    for copy in copies:
        copy.start()
    for copy in copies:
        copy.wait()


def fused(owners, peers, master_gate, master_up, router_weight, router_gain):
    experts, rows, width = master_gate.shape
    cut = width // peers
    tiles = width // LANES
    groups = 2 * experts // SUBLANES
    first, rest = -(-tiles // peers), -(-(groups - 1) * tiles // peers)
    depth = router_weight.shape[1]
    anywhere = pl.BlockSpec(memory_space=pl.ANY)
    vmem = pl.BlockSpec(memory_space=pltpu.VMEM)
    dma = pltpu.SemaphoreType.DMA
    turned = jax.ShapeDtypeStruct((experts, cut, rows * peers), jnp.bfloat16)

    def maxima(*shape):
        return (*shape, SUBLANES, LANES)

    gate, up, router, scales_first, scales_rest = pl.pallas_call(
        functools.partial(kernel, owners, peers),
        out_shape=(
            turned,
            turned,
            jax.ShapeDtypeStruct((depth * owners, rows * peers), jnp.bfloat16),
            jax.ShapeDtypeStruct(maxima(first * peers), jnp.float32),
            jax.ShapeDtypeStruct(maxima(rest * peers), jnp.float32),
        ),
        in_specs=[anywhere, anywhere, vmem, vmem],
        out_specs=(anywhere, anywhere, anywhere, vmem, vmem),
        scratch_shapes=[
            pltpu.VMEM((SLOTS, rows, width), jnp.float32),
            pltpu.VMEM(maxima(first * peers), jnp.float32),
            pltpu.VMEM(maxima(rest * peers), jnp.float32),
            pltpu.VMEM(maxima(peers, first), jnp.float32),
            pltpu.VMEM(maxima(peers, rest), jnp.float32),
            pltpu.VMEM((2, experts, width, rows), jnp.bfloat16),
            pltpu.VMEM((depth, rows), jnp.bfloat16),
            dma((SLOTS,)),
            dma((2, peers)),
            dma((2, peers)),
            dma((2, peers)),
            dma((2, peers)),
            dma((2, peers)),
            dma((2, peers)),
            dma((owners * peers,)),
            dma((owners * peers,)),
        ],
        compiler_params=pltpu.CompilerParams(
            has_side_effects=True,
            vmem_limit_bytes=(4 * experts + 4 * SLOTS) * rows * width + VMEM_FOR_REST,
        ),
    )(master_gate, master_up, router_weight.T, router_gain[None, :])
    landed = (gate, up, router, scales_first, scales_rest)
    gate, up, router, scales_first, scales_rest = pl.pallas_call(
        land,
        out_shape=[jax.ShapeDtypeStruct(a.shape, a.dtype) for a in landed],
        in_specs=[anywhere] * len(landed),
        out_specs=[pl.BlockSpec(memory_space=pltpu.HBM)] * len(landed),
        scratch_shapes=[dma((len(landed),))],
        compiler_params=pltpu.CompilerParams(vmem_limit_bytes=VMEM_FOR_REST),
        cost_estimate=pl.CostEstimate(
            flops=0, bytes_accessed=2 * sum(a.size for a in landed), transcendentals=0
        ),
    )(*landed)
    scales = jnp.concatenate([scales_first[:tiles], scales_rest[: (groups - 1) * tiles]])
    scales = scales.reshape(2, experts // SUBLANES, tiles, SUBLANES, LANES)
    scales = scales.transpose(0, 1, 3, 2, 4).reshape(2, experts, width)
    scales = lax.dynamic_slice_in_dim(scales, lax.axis_index("rows") * cut, cut, axis=2)
    return (
        gate.transpose(0, 2, 1),
        up.transpose(0, 2, 1),
        scales[0],
        scales[1],
        router.T,
    )


def plain(master_gate, master_up, router_weight, router_gain):
    scale_gate, scale_up = lax.pmax(
        (jnp.max(jnp.abs(master_gate), axis=1), jnp.max(jnp.abs(master_up), axis=1)), "rows"
    )
    narrow_gate, narrow_up = (
        (master_gate / jnp.expand_dims(scale_gate, 1)).astype(jnp.bfloat16),
        (master_up / jnp.expand_dims(scale_up, 1)).astype(jnp.bfloat16),
    )
    final_gate, final_up = (
        lax.all_to_all(narrow_gate, "rows", split_axis=2, concat_axis=1, tiled=True),
        lax.all_to_all(narrow_up, "rows", split_axis=2, concat_axis=1, tiled=True),
    )
    scale_gate = lax.dynamic_slice_in_dim(
        scale_gate, lax.axis_index("rows") * final_gate.shape[2], final_gate.shape[2], axis=1
    )
    scale_up = lax.dynamic_slice_in_dim(
        scale_up, lax.axis_index("rows") * final_up.shape[2], final_up.shape[2], axis=1
    )
    part_router = (router_weight * router_gain[:, None]).astype(jnp.bfloat16)
    row_router = lax.all_gather(part_router, "rows", axis=0, tiled=True)
    serve_router = lax.all_gather(row_router, "owner", axis=1, tiled=True)
    return (final_gate, final_up, scale_gate, scale_up, serve_router)


def solution(mesh):
    owners, peers = mesh.shape["owner"], mesh.shape["rows"]

    def shards(master_gate, master_up, router_weight, router_gain):
        experts, rows, width = master_gate.shape
        whole_tiles = (
            rows % LANES == 0
            and width % LANES == 0
            and width % (peers * PACKED) == 0
            and experts % SUBLANES == 0
            and experts >= SLOTS
            and experts % PER_SEND == 0
            and router_weight.shape[1] % PACKED == 0
            and (4 * experts + 4 * SLOTS) * rows * width <= VMEM_FOR_BLOCKS
        )
        run = functools.partial(fused, owners, peers) if whole_tiles else plain
        return run(master_gate, master_up, router_weight, router_gain)

    return jax.shard_map(
        shards,
        mesh=mesh,
        in_specs=(
            P("owner", "rows", None),
            P("owner", "rows", None),
            P("rows", "owner"),
            P("rows"),
        ),
        out_specs=(
            P("owner", None, "rows"),
            P("owner", None, "rows"),
            P("owner", "rows"),
            P("owner", "rows"),
            P(),
        ),
        check_vma=False,
    )
```

```python
import functools

import jax
import jax.numpy as jnp
from jax import lax
from jax.experimental import pallas as pl
from jax.experimental.pallas import tpu as pltpu
from jax.sharding import PartitionSpec as P

MESH = pl.DeviceIdType.MESH
LANES = 128
SUBLANES = 8
PACKED = 16
SLOTS = 4
PER_SEND = 2
VMEM_FOR_BLOCKS = 48 * 1024 * 1024
VMEM_FOR_REST = 2 * 1024 * 1024


def kernel(
    owners,
    peers,
    gate,
    up,
    router,
    gain,
    out_gate,
    out_up,
    out_router,
    scales_first,
    scales_rest,
    slots,
    largest_first,
    largest_rest,
    parts_first,
    parts_rest,
    send,
    row,
    slot_sem,
    send_sem,
    recv_sem,
    part_send,
    part_recv,
    whole_send,
    whole_recv,
    router_send,
    router_recv,
):
    owner, me = lax.axis_index("owner"), lax.axis_index("rows")
    experts, rows, width = gate.shape
    tiles = width // LANES
    cut = width // peers
    masters, outs = (gate, up), (out_gate, out_up)
    largest, parts = (largest_first, largest_rest), (parts_first, parts_rest)
    scales = (scales_first, scales_rest)
    lanes = pl.ds(pl.multiple_of(me * rows, LANES), rows)

    pairs = peers & (peers - 1) == 0

    def partner(k):
        if not pairs:
            return lax.rem(me + k, peers)
        bits = [1 << b for b in range(peers.bit_length() - 1) if k >> b & 1]
        return sum((bit - 2 * bit * lax.rem(me // bit, 2) for bit in bits), me)

    def origin(k):
        return partner(k) if pairs else lax.rem(me + peers - k, peers)

    def fetch(m, first, i):
        s = lax.rem(i, SLOTS)
        return pltpu.make_async_copy(masters[m].at[first + i], slots.at[s], slot_sem.at[s])

    def begin(m, first, length):
        for i in range(min(SLOTS, length)):
            fetch(m, first, i).start()

    def advance(m, first, length, i):
        if length > SLOTS:

            @pl.when(i + SLOTS < length)
            def _():
                fetch(m, first, i + SLOTS).start()

    def place(m, e, c, first):
        k = m * experts + e - (0 if first else SUBLANES)
        return (k // SUBLANES) * tiles + c, pl.ds(lax.rem(k, SUBLANES), 1)

    def maxima(m, first, length):
        stage = 0 if m == 0 and first < SUBLANES else 1

        def body(i, _):
            fetch(m, first, i).wait()
            for c in range(tiles):
                x = slots[lax.rem(i, SLOTS), :, c * LANES : (c + 1) * LANES]
                tile, sub = place(m, first + i, c, stage == 0)
                largest[stage][tile, sub, :] = jnp.max(jnp.abs(x), axis=0, keepdims=True)
            advance(m, first, length, i)
            return 0

        lax.fori_loop(0, length, body, 0)

    def part_copy(stage, k):
        per = parts[stage].shape[1]
        to = partner(k)
        return pltpu.make_async_remote_copy(
            src_ref=largest[stage].at[pl.ds(to * per, per)],
            dst_ref=parts[stage].at[k],
            send_sem=part_send.at[stage, k],
            recv_sem=part_recv.at[stage, k],
            device_id={"rows": to},
            device_id_type=MESH,
        )

    def share(stage, of):
        per = parts[stage].shape[1]
        return scales[stage].at[pl.ds(of * per, per)]

    def whole_copy(stage, k):
        return pltpu.make_async_remote_copy(
            src_ref=share(stage, me),
            dst_ref=share(stage, me),
            send_sem=whole_send.at[stage, k],
            recv_sem=whole_recv.at[stage, k],
            device_id={"rows": partner(k)},
            device_id_type=MESH,
        )

    order = sorted(range(1, peers), key=lambda k: (k.bit_length(), k))

    def scatter(stage):
        for k in order:
            part_copy(stage, k).start()

    def reduce(stage):
        per = parts[stage].shape[1]
        total = largest[stage][pl.ds(me * per, per)]
        for k in order:
            part_copy(stage, k).wait_recv()
            total = jnp.maximum(total, parts[stage][k])
        share(stage, me)[...] = total
        for k in order:
            whole_copy(stage, k).start()

    def gathered(stage):
        for k in order:
            part_copy(stage, k).wait_send()
            there = share(stage, origin(k))
            pltpu.make_async_copy(there, there, whole_recv.at[stage, k]).wait()
            whole_copy(stage, k).wait_send()

    def send_copy(m, k, e, length):
        to = partner(k)
        return pltpu.make_async_remote_copy(
            src_ref=send.at[m, pl.ds(e, length), pl.ds(pl.multiple_of(to * cut, PACKED), cut), :],
            dst_ref=outs[m].at[pl.ds(e, length), :, lanes],
            send_sem=send_sem.at[m, k],
            recv_sem=recv_sem.at[m, k],
            device_id={"rows": to},
            device_id_type=MESH,
        )

    def keep_copy(m, e, length):
        return pltpu.make_async_copy(
            send.at[m, pl.ds(e, length), pl.ds(pl.multiple_of(me * cut, PACKED), cut), :],
            outs[m].at[pl.ds(e, length), :, lanes],
            send_sem.at[m, 0],
        )

    def bulk(m, first, length, batch):
        stage = 0 if m == 0 and first < SUBLANES else 1

        def body(step, _):
            for j in range(batch):
                i = step * batch + j
                fetch(m, first, i).wait()
                for c in range(tiles):
                    x = slots[lax.rem(i, SLOTS), :, c * LANES : (c + 1) * LANES]
                    tile, sub = place(m, first + i, c, stage == 0)
                    s = scales[stage][tile, sub, :]
                    send[m, first + i, c * LANES : (c + 1) * LANES, :] = (x / s).T.astype(send.dtype)
                advance(m, first, length, i)
            for k in order:
                send_copy(m, k, first + step * batch, batch).start()
            keep_copy(m, first + step * batch, batch).start()
            return 0

        lax.fori_loop(0, length // batch, body, 0)

    depth = router.shape[0]
    block = out_router.at[pl.ds(pl.multiple_of(owner * depth, PACKED), depth), lanes]
    flat = owner * peers + me
    count = owners * peers

    def router_copy(k):
        to = lax.rem(flat + k, count)
        return pltpu.make_async_remote_copy(
            src_ref=row,
            dst_ref=block,
            send_sem=router_send.at[k],
            recv_sem=router_recv.at[k],
            device_id={"owner": to // peers, "rows": lax.rem(to, peers)},
            device_id_type=MESH,
        )

    def router_start(k, _):
        router_copy(k).start()
        return 0

    def router_wait(k, _):
        router_copy(k).wait()
        return 0

    barrier = pltpu.get_barrier_semaphore()

    def greet(k, _):
        to = lax.rem(flat + k, count)
        pl.semaphore_signal(
            barrier,
            inc=1,
            device_id={"owner": to // peers, "rows": lax.rem(to, peers)},
            device_id_type=MESH,
        )
        return 0

    begin(0, 0, SUBLANES)
    lax.fori_loop(1, count, greet, 0)
    largest_first[...] = jnp.zeros_like(largest_first)
    largest_rest[...] = jnp.zeros_like(largest_rest)
    row[...] = (router[...] * gain[...]).astype(row.dtype)
    maxima(0, 0, SUBLANES)
    pl.semaphore_wait(barrier, count - 1)
    scatter(0)
    begin(0, 0, 2)
    reduce(0)
    gathered(0)
    bulk(0, 0, 2, 1)
    if experts > SUBLANES:
        begin(0, SUBLANES, experts - SUBLANES)
        maxima(0, SUBLANES, experts - SUBLANES)
    begin(1, 0, experts)
    maxima(1, 0, experts)
    scatter(1)
    begin(0, 2, 2)
    bulk(0, 2, 2, 2)
    begin(0, 4, SUBLANES - 4)
    reduce(1)
    bulk(0, 4, SUBLANES - 4, PER_SEND)
    if experts > SUBLANES:
        begin(0, SUBLANES, experts - SUBLANES)
    gathered(1)
    if experts > SUBLANES:
        bulk(0, SUBLANES, experts - SUBLANES, PER_SEND)
    begin(1, 0, experts)
    lax.fori_loop(1, count, router_start, 0)
    keep_router = pltpu.make_async_copy(row, block, router_send.at[0])
    keep_router.start()
    bulk(1, 0, experts, PER_SEND)

    keep_router.wait()
    lax.fori_loop(1, count, router_wait, 0)
    for m in range(2):
        keep_copy(m, 0, experts).wait()
        for k in range(1, peers):
            send_copy(m, k, 0, experts).wait()


def land(*refs):
    arrays = len(refs) // 2
    ins, outs, sem = refs[:arrays], refs[arrays:-1], refs[-1]
    copies = [pltpu.make_async_copy(a, b, sem.at[i]) for i, (a, b) in enumerate(zip(ins, outs))]
    for copy in copies:
        copy.start()
    for copy in copies:
        copy.wait()


def fused(owners, peers, master_gate, master_up, router_weight, router_gain):
    experts, rows, width = master_gate.shape
    cut = width // peers
    tiles = width // LANES
    groups = 2 * experts // SUBLANES
    first, rest = -(-tiles // peers), -(-(groups - 1) * tiles // peers)
    depth = router_weight.shape[1]
    anywhere = pl.BlockSpec(memory_space=pl.ANY)
    vmem = pl.BlockSpec(memory_space=pltpu.VMEM)
    dma = pltpu.SemaphoreType.DMA
    turned = jax.ShapeDtypeStruct((experts, cut, rows * peers), jnp.bfloat16)

    def maxima(*shape):
        return (*shape, SUBLANES, LANES)

    gate, up, router, scales_first, scales_rest = pl.pallas_call(
        functools.partial(kernel, owners, peers),
        out_shape=(
            turned,
            turned,
            jax.ShapeDtypeStruct((depth * owners, rows * peers), jnp.bfloat16),
            jax.ShapeDtypeStruct(maxima(first * peers), jnp.float32),
            jax.ShapeDtypeStruct(maxima(rest * peers), jnp.float32),
        ),
        in_specs=[anywhere, anywhere, vmem, vmem],
        out_specs=(anywhere, anywhere, anywhere, vmem, vmem),
        scratch_shapes=[
            pltpu.VMEM((SLOTS, rows, width), jnp.float32),
            pltpu.VMEM(maxima(first * peers), jnp.float32),
            pltpu.VMEM(maxima(rest * peers), jnp.float32),
            pltpu.VMEM(maxima(peers, first), jnp.float32),
            pltpu.VMEM(maxima(peers, rest), jnp.float32),
            pltpu.VMEM((2, experts, width, rows), jnp.bfloat16),
            pltpu.VMEM((depth, rows), jnp.bfloat16),
            dma((SLOTS,)),
            dma((2, peers)),
            dma((2, peers)),
            dma((2, peers)),
            dma((2, peers)),
            dma((2, peers)),
            dma((2, peers)),
            dma((owners * peers,)),
            dma((owners * peers,)),
        ],
        compiler_params=pltpu.CompilerParams(
            collective_id=0,
            has_side_effects=True,
            vmem_limit_bytes=(4 * experts + 4 * SLOTS) * rows * width + VMEM_FOR_REST,
        ),
    )(master_gate, master_up, router_weight.T, router_gain[None, :])
    landed = (gate, up, router, scales_first, scales_rest)
    gate, up, router, scales_first, scales_rest = pl.pallas_call(
        land,
        out_shape=[jax.ShapeDtypeStruct(a.shape, a.dtype) for a in landed],
        in_specs=[anywhere] * len(landed),
        out_specs=[pl.BlockSpec(memory_space=pltpu.HBM)] * len(landed),
        scratch_shapes=[dma((len(landed),))],
        compiler_params=pltpu.CompilerParams(vmem_limit_bytes=VMEM_FOR_REST),
        cost_estimate=pl.CostEstimate(
            flops=0, bytes_accessed=2 * sum(a.size for a in landed), transcendentals=0
        ),
    )(*landed)
    scales = jnp.concatenate([scales_first[:tiles], scales_rest[: (groups - 1) * tiles]])
    scales = scales.reshape(2, experts // SUBLANES, tiles, SUBLANES, LANES)
    scales = scales.transpose(0, 1, 3, 2, 4).reshape(2, experts, width)
    scales = lax.dynamic_slice_in_dim(scales, lax.axis_index("rows") * cut, cut, axis=2)
    return (
        gate.transpose(0, 2, 1),
        up.transpose(0, 2, 1),
        scales[0],
        scales[1],
        router.T,
    )


def plain(master_gate, master_up, router_weight, router_gain):
    scale_gate, scale_up = lax.pmax(
        (jnp.max(jnp.abs(master_gate), axis=1), jnp.max(jnp.abs(master_up), axis=1)), "rows"
    )
    narrow_gate, narrow_up = (
        (master_gate / jnp.expand_dims(scale_gate, 1)).astype(jnp.bfloat16),
        (master_up / jnp.expand_dims(scale_up, 1)).astype(jnp.bfloat16),
    )
    final_gate, final_up = (
        lax.all_to_all(narrow_gate, "rows", split_axis=2, concat_axis=1, tiled=True),
        lax.all_to_all(narrow_up, "rows", split_axis=2, concat_axis=1, tiled=True),
    )
    scale_gate = lax.dynamic_slice_in_dim(
        scale_gate, lax.axis_index("rows") * final_gate.shape[2], final_gate.shape[2], axis=1
    )
    scale_up = lax.dynamic_slice_in_dim(
        scale_up, lax.axis_index("rows") * final_up.shape[2], final_up.shape[2], axis=1
    )
    part_router = (router_weight * router_gain[:, None]).astype(jnp.bfloat16)
    row_router = lax.all_gather(part_router, "rows", axis=0, tiled=True)
    serve_router = lax.all_gather(row_router, "owner", axis=1, tiled=True)
    return (final_gate, final_up, scale_gate, scale_up, serve_router)


def solution(mesh):
    owners, peers = mesh.shape["owner"], mesh.shape["rows"]

    def shards(master_gate, master_up, router_weight, router_gain):
        experts, rows, width = master_gate.shape
        whole_tiles = (
            rows % LANES == 0
            and width % LANES == 0
            and width % (peers * PACKED) == 0
            and experts % SUBLANES == 0
            and experts >= SLOTS
            and experts % PER_SEND == 0
            and router_weight.shape[1] % PACKED == 0
            and (4 * experts + 4 * SLOTS) * rows * width <= VMEM_FOR_BLOCKS
        )
        run = functools.partial(fused, owners, peers) if whole_tiles else plain
        return run(master_gate, master_up, router_weight, router_gain)

    return jax.shard_map(
        shards,
        mesh=mesh,
        in_specs=(
            P("owner", "rows", None),
            P("owner", "rows", None),
            P("rows", "owner"),
            P("rows"),
        ),
        out_specs=(
            P("owner", None, "rows"),
            P("owner", None, "rows"),
            P("owner", "rows"),
            P("owner", "rows"),
            P(),
        ),
        check_vma=False,
    )
```
